256 devices in a mesh: lat: 16 (over x, y), lon: 16 (over z, core).
Axes of the slice: x: 4, y: 4, z: 8, core: 2. Of those that a mesh axis runs over, the one named last changes fastest.
Arguments:
- transport: bfloat16 [48, 2048, 6144], P(None, 'lat', 'lon'), may hold values from -0.046875 to 0.046875
- sigma_class: int32 [48, 2048, 6144], P(None, 'lat', 'lon'), may hold values from 0 to 199
- basin_id: int32 [2048, 6144], P('lat', 'lon'), may hold values from 0 to 3
- depth_levels: int32 [2048, 6144], P('lat', 'lon'), may hold values from 0 to 48
Outputs:
- overturning: bfloat16 [4, 200, 2048], replicated
The draws below stay inside these ranges and needn't reach their ends.
Inputs may be any that keep to these rules, and one draw needn't show every extreme that they name: `depth_levels`: 0 marks a land column.
All inputs are finite; a program needn't handle non-finite values.
Results may differ from the reference program's by a relative error of at most 0.001.
Values may be sent and summed in bfloat16 or wider, within the bound.
No kernel may reach another device: no remote copies, remote signals or barrier semaphores. Data moves between devices by JAX's collectives and lax.ppermute only.
A program may use at most 64 MiB of HBM per device.

```python
import jax
import jax.numpy as jnp
from jax import lax

CLASSES = 200
BASINS = 4
ROWS_DEV = 128
COLS_DEV = 384
LEVELS = 48
NJ = 2048
NI = 6144
N_LON = 16


def touch_ends(values, own_key, low, high):
    longest = values.shape.index(max(values.shape))
    spots = []
    for shift in (0, 1):
        where = [jax.random.randint(jax.random.fold_in(own_key, axis), (), 0, length) for axis, length in enumerate(values.shape)]
        where[longest] = (where[longest] + shift) % values.shape[longest]
        spots.append(tuple(where))
    return values.at[spots[0]].set(low).at[spots[1]].set(high)


def steps_of(key, dims, cuts, low, largest):
    def one(dim, shards_of):
        draws = jax.random.uniform(jax.random.fold_in(jax.random.fold_in(key, 6), dim), (shards_of,), jnp.float32, low / len(cuts), largest / len(cuts))
        return jnp.repeat(jnp.exp(draws), dims[dim] // shards_of).reshape((-1,) + (1,) * (len(dims) - dim - 1))

    factor_of = one(*cuts[0])
    for cut in cuts[1:]:
        factor_of = factor_of * one(*cut)
    return factor_of


def bell_draw(key, extent, deviation, reach, split=(), held_as=jnp.bfloat16):
    result = jax.random.normal(key, extent, jnp.float32) * deviation
    if len(split) > 0:
        result = steps_of(key, extent, split, -0.22, 0.18) * result
    return jnp.clip(result, min=-reach, max=reach).astype(held_as)


def setup_inputs(seed: int = 0) -> dict:
    key_of = jax.random.split(jax.random.key(seed), 5)
    return {
        "transport": bell_draw(key_of[0], (LEVELS, NJ, NI), (2.0 / (COLS_DEV * N_LON * LEVELS / BASINS) ** 0.5), 0.046875, ((1, 16), (2, 16))),
        "sigma_class": touch_ends(jax.random.randint(key_of[1], (LEVELS, NJ, NI), 0, CLASSES), jax.random.fold_in(key_of[1], 1), 0, CLASSES - 1).astype(jnp.int32),
        "basin_id": touch_ends(jax.random.randint(key_of[2], (NJ, NI), 0, BASINS), jax.random.fold_in(key_of[2], 1), 0, BASINS - 1).astype(jnp.int32),
        "depth_levels": touch_ends(jax.random.randint(key_of[3], (NJ, NI), 0, LEVELS + 1), jax.random.fold_in(key_of[3], 1), 0, LEVELS).astype(jnp.int32),
    }


def bin_block(transport, sigma_class, basin_id, depth_levels):
    depth_count, row_count, col_count = sigma_class.shape
    level_index = lax.broadcasted_iota(jnp.int32, (depth_count, row_count, col_count), 0)
    row_index = lax.broadcasted_iota(jnp.int32, (depth_count, row_count, col_count), 1)
    wet_cells = level_index < depth_levels[None, :, :]
    weights = jnp.where(wet_cells, transport.astype(jnp.float32), jnp.float32(0.0))
    bin_index = ((basin_id[None, :, :] * CLASSES + sigma_class) * row_count + row_index).astype(jnp.int32)
    flat = jax.ops.segment_sum(weights.reshape(-1), bin_index.reshape(-1), num_segments=BASINS * CLASSES * row_count)
    return flat.reshape(BASINS, CLASSES, row_count)


def reference(transport, sigma_class, basin_id, depth_levels):
    block_count = NJ // ROWS_DEV

    def one_block(start):
        return bin_block(
            lax.dynamic_slice_in_dim(transport, start, ROWS_DEV, 1),
            lax.dynamic_slice_in_dim(sigma_class, start, ROWS_DEV, 1),
            lax.dynamic_slice_in_dim(basin_id, start, ROWS_DEV, 0),
            lax.dynamic_slice_in_dim(depth_levels, start, ROWS_DEV, 0),
        )

    starts = (jnp.arange(block_count) * ROWS_DEV).astype(jnp.int32)
    tables = lax.map(one_block, starts)
    table = jnp.transpose(tables, (1, 2, 0, 3)).reshape(BASINS, CLASSES, NJ)
    return jnp.cumsum(table, axis=1).astype(jnp.bfloat16)
```

```python
import functools

import jax
import jax.numpy as jnp
from jax import lax
from jax.experimental import pallas as pl
from jax.experimental.pallas import tpu as pltpu
from jax.sharding import Mesh, PartitionSpec as P

f32, bf16, i32 = jnp.float32, jnp.bfloat16, jnp.int32
CLASSES, BASINS = 200, 4
PAD = 224


def kernel(rows_unroll, flow_ref, class_ref, basin_ref, depth_ref, out_ref, high, low, weight, table):
    levels, block, cols = class_ref.shape
    step = pl.program_id(0)
    basin8 = basin_ref[...] * 8
    depth = depth_ref[...]
    for k in range(levels):
        klass = class_ref[k]
        high[k] = (basin8 + (klass >> 5)).astype(f32)
        low[k] = (klass & 31).astype(f32)
        weight[k] = jnp.where(depth > k, flow_ref[k].astype(f32), 0.0)
    iota = lax.broadcasted_iota(i32, (16, cols), 0).astype(f32)
    first, second = iota.astype(bf16), (iota + 16.0).astype(bf16)
    one, zero = jnp.ones((16, cols), bf16), jnp.zeros((16, cols), bf16)

    def wide(ref, k, row):
        return jnp.broadcast_to(ref[k, pl.ds(row, 1), :], (16, cols)).astype(bf16)

    def one_row(row):
        left, right = [], []
        for k in range(levels):
            hi, lo, w = wide(high, k, row), wide(low, k, row), wide(weight, k, row)
            left.append(jnp.concatenate([jnp.where(hi == first, w, zero), jnp.where(hi == second, w, zero)], 0))
            right.append(jnp.concatenate([jnp.where(lo <= first, one, zero), jnp.where(lo <= second, one, zero)], 0))
        left, right = jnp.concatenate(left, 1), jnp.concatenate(right, 1)
        return lax.dot_general(left, right, (((1,), (1,)), ((), ())), preferred_element_type=f32)

    def rows(i, _):
        for u in range(rows_unroll):
            row = i * rows_unroll + u
            table[step * block + row, :, 0:32] = one_row(row)
        return 0

    lax.fori_loop(0, block // rows_unroll, rows, 0)

    @pl.when(step == pl.num_programs(0) - 1)
    def _():
        for b in range(4):
            before = jnp.zeros((1, out_ref.shape[1]), f32)
            for hi in range(7):
                part = jnp.transpose(table[:, b * 8 + hi, :])[0:32]
                out_ref[b * PAD + hi * 32:b * PAD + hi * 32 + 32, :] = part + before
                before = before + part[31:32]


def bin_rows(transport, sigma_class, basin_id, depth_levels, block=8, rows_unroll=2):
    levels, row_count, cols = sigma_class.shape
    cube = pl.BlockSpec((levels, block, cols), lambda i: (0, i, 0))
    flat = pl.BlockSpec((block, cols), lambda i: (i, 0))
    return pl.pallas_call(
        functools.partial(kernel, rows_unroll),
        grid=(row_count // block,),
        in_specs=[cube, cube, flat, flat],
        out_specs=pl.BlockSpec((4 * PAD, row_count), lambda i: (0, 0)),
        out_shape=jax.ShapeDtypeStruct((4 * PAD, row_count), f32),
        scratch_shapes=[pltpu.VMEM((levels, block, cols), f32)] * 3 + [pltpu.VMEM((row_count, 32, 128), f32)],
        compiler_params=pltpu.CompilerParams(vmem_limit_bytes=60000 * 1024),
        name="bin_rows",
    )(transport, sigma_class, basin_id, depth_levels)


def shift(array, axis, by, size):
    return lax.ppermute(array, axis, [(i, (i + by) % size) for i in range(size)])


def fold(array, axis, bit, size):
    upper = (lax.axis_index(axis) & bit) > 0
    half = array.shape[0] // 2
    low, high = array[:half], array[half:]
    sent = lax.ppermute(jnp.where(upper, low, high), axis, [(i, i ^ bit) for i in range(size)])
    return jnp.where(upper, high, low) + sent


def double(array, axis, bit, size):
    upper = (lax.axis_index(axis) & bit) > 0
    other = lax.ppermute(array, axis, [(i, i ^ bit) for i in range(size)])
    return jnp.concatenate([jnp.where(upper, other, array), jnp.where(upper, array, other)], 0)


def ring4(array, axis):
    me = lax.axis_index(axis)
    rows, width = array.shape
    others = [(array, me)] + [(shift(array, axis, by, 4), (me - by) % 4) for by in (1, 3, 2)]
    out = jnp.zeros((rows, 4 * width), array.dtype)
    for piece, where in others:
        out = lax.dynamic_update_slice(out, piece, (0, where * width))
    return out


def reduce_z(mine):
    return lax.all_to_all(mine.reshape(8, 56, 128), "z", 0, 0, tiled=True).reshape(8, 56, 128).sum(0)


def body(transport, sigma_class, basin_id, depth_levels):
    table = bin_rows(transport, sigma_class, basin_id, depth_levels)
    mine = fold(table, "core", 1, 2)
    total = reduce_z(mine).astype(bf16)
    for bit in (4, 2, 1):
        total = total[None] if bit == 4 else total
        total = double(total, "z", bit, 8)
    both = unscramble(total)
    a, b = both[0, :CLASSES], both[1, :CLASSES]
    a1, b1 = ring4(a, "y"), ring4(b, "x")
    a2 = ring4(a1, "x")
    b2 = ring4(b1, "y")
    b2 = b2.reshape(CLASSES, 4, 4, 128).swapaxes(1, 2).reshape(CLASSES, 2048)
    pair = jnp.stack([a2, b2])
    other = shift(pair, "core", 1, 2)
    core = lax.axis_index("core")
    out = jnp.zeros((BASINS, CLASSES, 2048), bf16)
    out = lax.dynamic_update_slice(out, pair, (2 * core, 0, 0))
    return lax.dynamic_update_slice(out, other, (2 * (1 - core), 0, 0))


def unscramble(total):
    return total.reshape(2, 2, 2, 56, 128).transpose(2, 1, 0, 3, 4).reshape(2, PAD, 128)


def solution(mesh):
    fine = Mesh(mesh.devices.reshape(4, 4, 8, 2), ("x", "y", "z", "core"))
    lat, lon = ("x", "y"), ("z", "core")
    placed = (P(None, lat, lon), P(None, lat, lon), P(lat, lon), P(lat, lon))
    return jax.shard_map(body, mesh=fine, in_specs=placed, out_specs=P(), check_vma=False)
```

```python
import functools

import jax
import jax.numpy as jnp
from jax import lax
from jax.experimental import pallas as pl
from jax.experimental.pallas import tpu as pltpu
from jax.sharding import Mesh, PartitionSpec as P

f32, bf16, i32 = jnp.float32, jnp.bfloat16, jnp.int32
CLASSES, BASINS = 200, 4
PAD = 224


def kernel(rows_unroll, flow_ref, class_ref, basin_ref, depth_ref, out_ref, high, low, weight, table):
    levels, block, cols = class_ref.shape
    step = pl.program_id(0)
    basin8 = basin_ref[...] * 8
    depth = depth_ref[...]
    for k in range(levels):
        klass = class_ref[k]
        high[k] = (basin8 + (klass >> 5)).astype(f32)
        low[k] = (klass & 31).astype(f32)
        weight[k] = jnp.where(depth > k, flow_ref[k].astype(f32), 0.0)
    iota = lax.broadcasted_iota(i32, (16, cols), 0).astype(f32)
    first, second = iota.astype(bf16), (iota + 16.0).astype(bf16)
    one, zero = jnp.ones((16, cols), bf16), jnp.zeros((16, cols), bf16)

    def wide(ref, k, row):
        return jnp.broadcast_to(ref[k, pl.ds(row, 1), :], (16, cols)).astype(bf16)

    def one_row(row):
        left, right = [], []
        for k in range(levels):
            hi, lo, w = wide(high, k, row), wide(low, k, row), wide(weight, k, row)
            left.append(jnp.concatenate([jnp.where(hi == first, w, zero), jnp.where(hi == second, w, zero)], 0))
            right.append(jnp.concatenate([jnp.where(lo <= first, one, zero), jnp.where(lo <= second, one, zero)], 0))
        left, right = jnp.concatenate(left, 1), jnp.concatenate(right, 1)
        return lax.dot_general(left, right, (((1,), (1,)), ((), ())), preferred_element_type=f32)

    def rows(i, _):
        for u in range(rows_unroll):
            row = i * rows_unroll + u
            table[step * block + row, :, 0:32] = one_row(row)
        return 0

    lax.fori_loop(0, block // rows_unroll, rows, 0)

    @pl.when(step == pl.num_programs(0) - 1)
    def _():
        for b in range(4):
            before = jnp.zeros((1, out_ref.shape[1]), f32)
            for hi in range(7):
                part = jnp.transpose(table[:, b * 8 + hi, :])[0:32]
                out_ref[b * PAD + hi * 32:b * PAD + hi * 32 + 32, :] = part + before
                before = before + part[31:32]


def bin_rows(transport, sigma_class, basin_id, depth_levels, block=8, rows_unroll=8):
    levels, row_count, cols = sigma_class.shape
    cube = pl.BlockSpec((levels, block, cols), lambda i: (0, i, 0))
    flat = pl.BlockSpec((block, cols), lambda i: (i, 0))
    return pl.pallas_call(
        functools.partial(kernel, rows_unroll),
        grid=(row_count // block,),
        in_specs=[cube, cube, flat, flat],
        out_specs=pl.BlockSpec((4 * PAD, row_count), lambda i: (0, 0)),
        out_shape=jax.ShapeDtypeStruct((4 * PAD, row_count), f32),
        scratch_shapes=[pltpu.VMEM((levels, block, cols), f32)] * 3 + [pltpu.VMEM((row_count, 32, 128), f32)],
        compiler_params=pltpu.CompilerParams(vmem_limit_bytes=60000 * 1024),
        name="bin_rows",
    )(transport, sigma_class, basin_id, depth_levels)


def shift(array, axis, by, size):
    return lax.ppermute(array, axis, [(i, (i + by) % size) for i in range(size)])


def fold(array, axis, bit, size):
    upper = (lax.axis_index(axis) & bit) > 0
    half = array.shape[0] // 2
    low, high = array[:half], array[half:]
    sent = lax.ppermute(jnp.where(upper, low, high), axis, [(i, i ^ bit) for i in range(size)])
    return jnp.where(upper, high, low) + sent


def double(array, axis, bit, size):
    upper = (lax.axis_index(axis) & bit) > 0
    other = lax.ppermute(array, axis, [(i, i ^ bit) for i in range(size)])
    return jnp.concatenate([jnp.where(upper, other, array), jnp.where(upper, array, other)], 0)


def ring4(array, axis):
    me = lax.axis_index(axis)
    rows, width = array.shape
    others = [(array, me)] + [(shift(array, axis, by, 4), (me - by) % 4) for by in (1, 3, 2)]
    out = jnp.zeros((rows, 4 * width), array.dtype)
    for piece, where in others:
        out = lax.dynamic_update_slice(out, piece, (0, where * width))
    return out


def reduce_z(mine):
    return lax.all_to_all(mine.reshape(8, 56, 128), "z", 0, 0, tiled=True).reshape(8, 56, 128).sum(0)


def gather(array, axis, size):
    return lax.all_to_all(jnp.broadcast_to(array[None], (size,) + array.shape), axis, 0, 0, tiled=True)


def body(transport, sigma_class, basin_id, depth_levels):
    table = bin_rows(transport, sigma_class, basin_id, depth_levels)
    mine = fold(table, "core", 1, 2)
    total = reduce_z(mine).astype(bf16)
    both = gather(total, "z", 8).reshape(2, PAD, 128)[:, :CLASSES]
    rows = gather(both, ("x", "y"), 16)
    other = shift(rows, "core", 1, 2)
    core = lax.axis_index("core")
    first = jnp.where(core == 0, rows, other)
    second = jnp.where(core == 0, other, rows)
    whole = jnp.concatenate([first, second], 1)
    return whole.transpose(1, 2, 0, 3).reshape(BASINS, CLASSES, 2048)


def solution(mesh):
    fine = Mesh(mesh.devices.reshape(4, 4, 8, 2), ("x", "y", "z", "core"))
    lat, lon = ("x", "y"), ("z", "core")
    placed = (P(None, lat, lon), P(None, lat, lon), P(lat, lon), P(lat, lon))
    return jax.shard_map(body, mesh=fine, in_specs=placed, out_specs=P(), check_vma=False)
```

```python
import functools

import jax
import jax.numpy as jnp
from jax import lax
from jax.experimental import pallas as pl
from jax.experimental.pallas import tpu as pltpu
from jax.sharding import Mesh, PartitionSpec as P

f32, bf16, i32 = jnp.float32, jnp.bfloat16, jnp.int32
CLASSES, BASINS = 200, 4
PAD = 224


def kernel(rows_unroll, core_ref, flow_ref, class_ref, basin_ref, depth_ref, keep_ref, send_ref, high, low, weight, table):
    levels, block, cols = class_ref.shape
    step = pl.program_id(0)
    basin8 = basin_ref[...] * 8
    depth = depth_ref[...]
    for k in range(levels):
        klass = class_ref[k]
        high[k] = (basin8 + (klass >> 5)).astype(f32)
        low[k] = (klass & 31).astype(f32)
        weight[k] = jnp.where(depth > k, flow_ref[k].astype(f32), 0.0)
    iota = lax.broadcasted_iota(i32, (16, cols), 0).astype(f32)
    first, second = iota.astype(bf16), (iota + 16.0).astype(bf16)
    one, zero = jnp.ones((16, cols), bf16), jnp.zeros((16, cols), bf16)

    def wide(ref, k, row):
        return jnp.broadcast_to(ref[k, pl.ds(row, 1), :], (16, cols)).astype(bf16)

    def one_row(row):
        left, right = [], []
        for k in range(levels):
            hi, lo, w = wide(high, k, row), wide(low, k, row), wide(weight, k, row)
            left.append(jnp.concatenate([jnp.where(hi == first, w, zero), jnp.where(hi == second, w, zero)], 0))
            right.append(jnp.concatenate([jnp.where(lo <= first, one, zero), jnp.where(lo <= second, one, zero)], 0))
        left, right = jnp.concatenate(left, 1), jnp.concatenate(right, 1)
        return lax.dot_general(left, right, (((1,), (1,)), ((), ())), preferred_element_type=f32)

    def rows(i, _):
        for u in range(rows_unroll):
            row = i * rows_unroll + u
            table[step * block + row, :, 0:32] = one_row(row)
        return 0

    lax.fori_loop(0, block // rows_unroll, rows, 0)

    @pl.when(step == pl.num_programs(0) - 1)
    def _():
        for b in range(4):
            before = jnp.zeros((1, keep_ref.shape[1]), f32)
            parts = []
            for hi in range(7):
                part = jnp.transpose(table[:, b * 8 + hi, :])[0:32]
                parts.append(part + before)
                before = before + part[31:32]
            whole = jnp.concatenate(parts, 0)
            own = core_ref[0] == b // 2
            rows_of = pl.ds((b % 2) * PAD, PAD)

            @pl.when(own)
            def _():
                keep_ref[rows_of, :] = whole

            @pl.when(jnp.logical_not(own))
            def _():
                send_ref[rows_of, :] = whole


def bin_rows(core, transport, sigma_class, basin_id, depth_levels, block=16, rows_unroll=16):
    levels, row_count, cols = sigma_class.shape
    cube = pl.BlockSpec((levels, block, cols), lambda i: (0, i, 0))
    flat = pl.BlockSpec((block, cols), lambda i: (i, 0))
    return pl.pallas_call(
        functools.partial(kernel, rows_unroll),
        grid=(row_count // block,),
        in_specs=[pl.BlockSpec(memory_space=pltpu.SMEM), cube, cube, flat, flat],
        out_specs=[pl.BlockSpec((2 * PAD, row_count), lambda i: (0, 0))] * 2,
        out_shape=[jax.ShapeDtypeStruct((2 * PAD, row_count), f32)] * 2,
        scratch_shapes=[pltpu.VMEM((levels, block, cols), f32)] * 3 + [pltpu.VMEM((row_count, 32, 128), f32)],
        compiler_params=pltpu.CompilerParams(vmem_limit_bytes=60000 * 1024),
        name="bin_rows",
    )(core, transport, sigma_class, basin_id, depth_levels)


def shift(array, axis, by, size):
    return lax.ppermute(array, axis, [(i, (i + by) % size) for i in range(size)])


def reduce_z(mine):
    return lax.all_to_all(mine.reshape(8, 56, 128), "z", 0, 0, tiled=True).reshape(8, 56, 128).sum(0)


def gather(array, axis, size):
    return lax.all_to_all(jnp.broadcast_to(array[None], (size,) + array.shape), axis, 0, 0, tiled=True)


def body(transport, sigma_class, basin_id, depth_levels):
    core = lax.axis_index("core")
    keep, send = bin_rows(core.reshape(1).astype(i32), transport, sigma_class, basin_id, depth_levels)
    mine = keep + shift(send, "core", 1, 2)
    total = reduce_z(mine).astype(bf16)
    both = gather(total, "z", 8).reshape(2, PAD, 128)[:, :CLASSES]
    rows = gather(both, ("x", "y"), 16)
    other = shift(rows, "core", 1, 2)
    first = jnp.where(core == 0, rows, other)
    second = jnp.where(core == 0, other, rows)
    whole = jnp.concatenate([first, second], 1)
    return whole.transpose(1, 2, 0, 3).reshape(BASINS, CLASSES, 2048)


def solution(mesh):
    fine = Mesh(mesh.devices.reshape(4, 4, 8, 2), ("x", "y", "z", "core"))
    lat, lon = ("x", "y"), ("z", "core")
    placed = (P(None, lat, lon), P(None, lat, lon), P(lat, lon), P(lat, lon))
    return jax.shard_map(body, mesh=fine, in_specs=placed, out_specs=P(), check_vma=False)
```

```python
import functools

import jax
import jax.numpy as jnp
from jax import lax
from jax.experimental import pallas as pl
from jax.experimental.pallas import tpu as pltpu
from jax.sharding import Mesh, PartitionSpec as P

f32, bf16, i32 = jnp.float32, jnp.bfloat16, jnp.int32
CLASSES, BASINS = 200, 4
PAD = 224


def kernel(rows_unroll, core_ref, flow_ref, class_ref, basin_ref, depth_ref, keep_ref, send_ref, high, low, weight, table):
    levels, block, cols = class_ref.shape
    step = pl.program_id(0)
    basin8 = basin_ref[...] * 8
    depth = depth_ref[...]
    for k in range(levels):
        klass = class_ref[k]
        high[k] = (basin8 + (klass >> 5)).astype(f32)
        low[k] = (klass & 31).astype(f32)
        weight[k] = jnp.where(depth > k, flow_ref[k].astype(f32), 0.0)
    iota = lax.broadcasted_iota(i32, (16, cols), 0).astype(f32)
    first, second = iota.astype(bf16), (iota + 16.0).astype(bf16)
    one, zero = jnp.ones((16, cols), bf16), jnp.zeros((16, cols), bf16)

    def wide(ref, k, row):
        return jnp.broadcast_to(ref[k, pl.ds(row, 1), :], (16, cols)).astype(bf16)

    def one_row(row):
        left, right = [], []
        for k in range(levels):
            hi, lo, w = wide(high, k, row), wide(low, k, row), wide(weight, k, row)
            left.append(jnp.concatenate([jnp.where(hi == first, w, zero), jnp.where(hi == second, w, zero)], 0))
            right.append(jnp.concatenate([jnp.where(lo <= first, one, zero), jnp.where(lo <= second, one, zero)], 0))
        left, right = jnp.concatenate(left, 1), jnp.concatenate(right, 1)
        return lax.dot_general(left, right, (((1,), (1,)), ((), ())), preferred_element_type=f32)

    def rows(i, _):
        for u in range(rows_unroll):
            row = i * rows_unroll + u
            table[step * block + row, :, 0:32] = one_row(row)
        return 0

    lax.fori_loop(0, block // rows_unroll, rows, 0)

    @pl.when(step == pl.num_programs(0) - 1)
    def _():
        for b in range(4):
            before = jnp.zeros((1, keep_ref.shape[1]), f32)
            parts = []
            for hi in range(7):
                part = jnp.transpose(table[:, b * 8 + hi, :])[0:32]
                parts.append(part + before)
                before = before + part[31:32]
            whole = jnp.concatenate(parts, 0)
            own = core_ref[0] == b // 2
            rows_of = pl.ds((b % 2) * PAD, PAD)

            @pl.when(own)
            def _():
                keep_ref[rows_of, :] = whole

            @pl.when(jnp.logical_not(own))
            def _():
                send_ref[rows_of, :] = whole


def bin_rows(core, transport, sigma_class, basin_id, depth_levels, block=16, rows_unroll=16):
    levels, row_count, cols = sigma_class.shape
    cube = pl.BlockSpec((levels, block, cols), lambda i: (0, i, 0))
    flat = pl.BlockSpec((block, cols), lambda i: (i, 0))
    return pl.pallas_call(
        functools.partial(kernel, rows_unroll),
        grid=(row_count // block,),
        in_specs=[pl.BlockSpec(memory_space=pltpu.SMEM), cube, cube, flat, flat],
        out_specs=[pl.BlockSpec((2 * PAD, row_count), lambda i: (0, 0))] * 2,
        out_shape=[jax.ShapeDtypeStruct((2 * PAD, row_count), f32)] * 2,
        scratch_shapes=[pltpu.VMEM((levels, block, cols), f32)] * 3 + [pltpu.VMEM((row_count, 32, 128), f32)],
        compiler_params=pltpu.CompilerParams(vmem_limit_bytes=60000 * 1024),
        name="bin_rows",
    )(core, transport, sigma_class, basin_id, depth_levels)


def shift(array, axis, by, size):
    return lax.ppermute(array, axis, [(i, (i + by) % size) for i in range(size)])


def reduce_z(mine):
    return lax.all_to_all(mine.reshape(8, 56, 128), "z", 0, 0, tiled=True).reshape(8, 56, 128).sum(0)


def gather(array, axis, size):
    return lax.all_to_all(jnp.broadcast_to(array[None], (size,) + array.shape), axis, 0, 0, tiled=True)


def body(transport, sigma_class, basin_id, depth_levels):
    core = lax.axis_index("core")
    keep, send = bin_rows(core.reshape(1).astype(i32), transport, sigma_class, basin_id, depth_levels)
    mine = keep + shift(send, "core", 1, 2)
    total = reduce_z(mine).astype(bf16)
    both = gather(total, "z", 8).reshape(2, PAD, 128)[:, :CLASSES]
    rows = gather(both, ("x", "y"), 16)
    other = shift(rows, "core", 1, 2)
    def placed_rows(out, part, at):
        return lax.dynamic_update_slice(out, part.transpose(1, 2, 0, 3).reshape(2, CLASSES, 2048), (2 * at, 0, 0))

    out = placed_rows(jnp.zeros((BASINS, CLASSES, 2048), bf16), rows, core)
    return placed_rows(out, other, 1 - core)


def solution(mesh):
    fine = Mesh(mesh.devices.reshape(4, 4, 8, 2), ("x", "y", "z", "core"))
    lat, lon = ("x", "y"), ("z", "core")
    placed = (P(None, lat, lon), P(None, lat, lon), P(lat, lon), P(lat, lon))
    return jax.shard_map(body, mesh=fine, in_specs=placed, out_specs=P(), check_vma=False)
```
